32 devices in a mesh: parts: 2 (over y), seq: 4 (over z), head: 2 (over x), rep: 2 (over core).
Axes of the slice: x: 2, y: 2, z: 4, core: 2. Of those that a mesh axis runs over, the one named last changes fastest.
Arguments:
- queries: bfloat16 [4, 1024, 2048], P(('parts', 'rep'), 'seq', 'head'), parts along dimension 0, may hold values from -6 to 6
- reflect_keys: bfloat16 [4, 1024, 2, 2048], P(('parts', 'rep'), 'seq', None, 'head'), parts along dimension 0, may hold values from -6 to 6
- reflect_values: bfloat16 [4, 1024, 2, 2048], P(('parts', 'rep'), 'seq', None, 'head'), parts along dimension 0, may hold values from -6 to 6
- reflect_beta: float32 [4, 1024, 2, 16], P(('parts', 'rep'), 'seq', None, 'head'), parts along dimension 0, may hold values from 0.2 to 2
- log_decay: float32 [4, 1024, 16], P(('parts', 'rep'), 'seq', 'head'), parts along dimension 0, may hold values from -2.5 to 0
- prompt_lengths: int32 [4, 6], P(('parts', 'rep')), parts along dimension 0, may hold values from 1 to 512, 1024 in all within a row
- norm_gain: float32 [128], replicated, may hold values from 0.1 to 1.9
- out_weight: bfloat16 [2048, 2048], P('head'), may hold values from -0.125 to 0.125
Outputs:
- layer_out: bfloat16 [4, 1024, 2048], P(('parts', 'rep'), ('seq', 'head')), parts along dimension 0
The draws below stay inside these ranges and needn't reach their ends.
There are 2 independent parts, one for each index of `parts`. The reference program is written for one: setup_inputs(seed, part) draws one part's arguments, and reference() takes and returns one part's arrays. A program takes and returns all parts, laid end to end along the dimension named above; an argument that names none is the same for every part. Nothing has to cross between parts.
Inputs may be any that keep to these rules, and one draw needn't show every extreme that they name: `prompt_lengths`: the 6 prompts of a pack lie end to end from its first token and cover all 1024 tokens; the longest has exactly 512.
All inputs are finite; a program needn't handle non-finite values.
Results may differ from the reference program's by a relative error of at most 0.0095.
Values may be sent and summed in bfloat16 or wider, within the bound.
A program may use at most 64 MiB of HBM per device.

```python
import math
import jax
import jax.numpy as jnp
import numpy as np
from jax import lax

D = 2048
HEADS = 16
DK = 128
REFL = 2
BLOCK = 64
DOCS = 6
TOK_DEV = 256
BUNDLE_COUNT = 2
BUNDLE_SPAN = 1024
MOST_LEN = 512
N_HEAD = 2


def slow_heads(key):
    chances = jax.random.uniform(jax.random.fold_in(key, 11), (HEADS,))
    return chances < 0.5


def draw_log_decay(key, part):
    slow_mask = slow_heads(key)
    slow_rate = jnp.exp(jax.random.uniform(jax.random.fold_in(key, 21), (HEADS,), minval=jnp.log(0.1 / MOST_LEN), maxval=jnp.log(1.0 / MOST_LEN)))
    fast_rate = jnp.exp(jax.random.uniform(jax.random.fold_in(key, 22), (HEADS,), minval=jnp.log(1.0 / 50.0), maxval=jnp.log(1.0 / 20.0)))
    channel_speed = jnp.where(slow_mask, slow_rate, fast_rate)
    uneven_quantity = jax.random.uniform(jax.random.fold_in(key, 23), (BUNDLE_COUNT, BUNDLE_SPAN, HEADS), minval=0.4, maxval=1.6)
    symbol_span = jnp.exp(jax.random.uniform(jax.random.fold_in(key, 24), (BUNDLE_COUNT, BUNDLE_SPAN // TOK_DEV, HEADS), minval=jnp.log(0.5), maxval=jnp.log(2.0)))
    symbol_span = jnp.repeat(symbol_span, TOK_DEV, axis=1)
    spike_position = jax.random.randint(jax.random.fold_in(key, 25), (BUNDLE_COUNT, 3), 0, BUNDLE_SPAN)
    spike_kept = jax.random.uniform(jax.random.fold_in(key, 26), (BUNDLE_COUNT, 3), minval=0.5, maxval=0.8)
    spike_hits = jnp.arange(BUNDLE_SPAN)[None, None, :] == spike_position[:, :, None]
    spike_log_scale = jnp.sum(jnp.where(spike_hits, jnp.log(spike_kept)[:, :, None], 0.0), axis=1)
    return (spike_log_scale[:, :, None] - channel_speed * uneven_quantity * symbol_span).astype(jnp.float32)


def draw_reflect_beta(key, part):
    slow_mask = slow_heads(key)
    margin = jnp.exp(jax.random.uniform(jax.random.fold_in(key, 31), (BUNDLE_COUNT, BUNDLE_SPAN, REFL, HEADS), minval=jnp.log(0.0001), maxval=jnp.log(0.02)))
    spread = jax.random.uniform(jax.random.fold_in(key, 32), (BUNDLE_COUNT, BUNDLE_SPAN, REFL, HEADS), minval=0.2, maxval=1.9)
    return jnp.where(slow_mask, 2.0 - margin, spread).astype(jnp.float32)


def shard_levels(rng, shape, pieces, least, top_value):
    gain, own = 1.0, jax.random.fold_in(rng, 6)
    for position, blocks in pieces:
        draws = jnp.exp(jax.random.uniform(jax.random.fold_in(own, position), (blocks,), jnp.float32, least / len(pieces), top_value / len(pieces)))
        gain = gain * jnp.repeat(draws, shape[position] // blocks).reshape([-1 if axis == position else 1 for axis in range(len(shape))])
    return gain


def profile(amount, total, reach, skew):
    loads = [(1 << 20) // math.isqrt(standing ** skew) + 1 for standing in range(2, amount + 1)]
    rest, holding = total - reach - (amount - 1), [1] * (amount - 1)
    while rest > 0:
        candidates = [i for i in range(amount - 1) if holding[i] < reach]
        pool, budget = sum([loads[i] for i in candidates]), rest
        for i in candidates:
            extra = min(reach - holding[i], max(1, budget * loads[i] // pool), rest)
            holding[i] = holding[i] + extra
            rest = rest - extra
    return np.array([reach] + holding)


def ragged(rng, count, total, limit, lean):
    if count == 2:
        one = jax.random.randint(rng, (), max(1, total - limit), min(limit, total - 1) + 1)
        return jnp.stack([one, total - one])
    tallies = jnp.asarray(profile(count, total, limit, lean), jnp.int32)
    twos = (count - 1) // 2
    donor, taker = tallies[1:1 + 2 * twos:2], tallies[2:2 + 2 * twos:2]
    room = jnp.minimum(donor - 1, limit - taker)
    moved = jax.random.randint(jax.random.fold_in(rng, 1), (twos,), 0, 1 << 20) % (room + 1)
    tallies = tallies.at[1:1 + 2 * twos:2].set(donor - moved).at[2:2 + 2 * twos:2].set(taker + moved)
    return tallies[jax.random.permutation(jax.random.fold_in(rng, 2), count)]


def scatter_about(key, extent, width, most, cuts=(), held_as=jnp.bfloat16):
    factor_of = shard_levels(key, extent, cuts, -0.22, 0.18) if cuts else 1.0
    entries = jax.random.normal(key, extent, jnp.float32) * width * factor_of
    return jnp.minimum(jnp.maximum(entries, -most), most).astype(held_as)


def setup_inputs(seed: int = 0, part: int = 0) -> dict:
    streams_of = jax.random.split(jax.random.key(seed), 9)
    own_keys = jax.random.split(jax.random.fold_in(streams_of[8], part), 9)
    queries = scatter_about(own_keys[0], (BUNDLE_COUNT, BUNDLE_SPAN, HEADS * DK), 1.0, 6.0, ((0, 2), (1, 4), (2, 2)))
    reflect_keys = scatter_about(own_keys[1], (BUNDLE_COUNT, BUNDLE_SPAN, REFL, HEADS * DK), 1.0, 6.0, ((0, 2), (1, 4), (3, 2)))
    reflect_values = scatter_about(own_keys[2], (BUNDLE_COUNT, BUNDLE_SPAN, REFL, HEADS * DK), 1.0, 6.0, ((0, 2), (1, 4), (3, 2)))
    reflect_beta = draw_reflect_beta(jax.random.fold_in(jax.random.fold_in(streams_of[8], part), 71), part)
    log_decay = draw_log_decay(jax.random.fold_in(jax.random.fold_in(streams_of[8], part), 71), part)
    prompt_lengths = jax.vmap(lambda own: ragged(own, DOCS, BUNDLE_SPAN, MOST_LEN, 2))(jax.random.split(own_keys[5], BUNDLE_COUNT)).reshape((BUNDLE_COUNT, DOCS)).astype(jnp.int32)
    norm_gain = jnp.clip(1.0 + 0.18 * jax.random.normal(streams_of[6], (DK,), jnp.float32), 0.1, 1.9)
    out_weight = scatter_about(streams_of[7], (HEADS * DK, D), (HEADS * DK) ** -0.5, 0.125, ((0, 2),))
    return dict(queries=queries, reflect_keys=reflect_keys, reflect_values=reflect_values, reflect_beta=reflect_beta, log_decay=log_decay, prompt_lengths=prompt_lengths, norm_gain=norm_gain, out_weight=out_weight)


highest = lax.Precision.HIGHEST
epsilon = 1e-06

def unit_rows(vectors):
    return vectors * lax.rsqrt(lax.optimization_barrier(jnp.sum(vectors * vectors, axis=-1, keepdims=True)) + epsilon)

def block_parts(key_rows, value_rows, beta_rows, decay_rows, seg_rows, seg_before):
    steps_here = key_rows.shape[-2]
    cum_decay = jnp.cumsum(decay_rows, axis=-1)
    ordinal = jnp.arange(steps_here)
    incl_mask = ordinal[:, None] >= ordinal[None, :]
    strict_mask = ordinal[:, None] > ordinal[None, :]
    same_doc = seg_rows[:, None, :, None] == seg_rows[:, None, None, :]
    decay_gap = cum_decay[..., :, None] - cum_decay[..., None, :]
    decay_ratio = jnp.where(incl_mask & same_doc, jnp.exp(jnp.minimum(decay_gap, 0.0)), 0.0)
    carry_in = jnp.where(seg_rows[:, None, :] == seg_before[:, None, None], jnp.exp(cum_decay), 0.0)
    key_inner = jnp.einsum('bhik,bhjk->bhij', key_rows, key_rows, precision=highest)
    system = jnp.eye(steps_here, dtype=key_rows.dtype) + jnp.where(strict_mask, beta_rows[..., :, None] * decay_ratio * key_inner, 0.0)
    right_side = jnp.concatenate([beta_rows[..., None] * value_rows, (beta_rows * carry_in)[..., None] * key_rows], axis=-1)
    solved = lax.linalg.triangular_solve(system, right_side, left_side=True, lower=True, unit_diagonal=True)
    val_width = value_rows.shape[-1]
    return (decay_ratio, carry_in, solved[..., :val_width], solved[..., val_width:])

def reference(queries, reflect_keys, reflect_values, reflect_beta, log_decay, prompt_lengths, norm_gain, out_weight):
    pack_count = queries.shape[0]
    length = queries.shape[1]
    blocks = length // BLOCK
    sub_steps = REFL * BLOCK
    doc_ends = jnp.cumsum(prompt_lengths, axis=-1).astype(jnp.int32)
    positions = jnp.arange(length, dtype=jnp.int32)
    segment = lax.optimization_barrier(jnp.sum((positions[None, :, None] >= doc_ends[:, None, :]).astype(jnp.int32), axis=-1)).astype(jnp.int32)
    query_rows = unit_rows(queries.astype(jnp.float32).reshape(pack_count, blocks, BLOCK, HEADS, DK)) * DK ** (-0.5)
    query_rows = query_rows.transpose(1, 0, 3, 2, 4)
    key_rows = unit_rows(reflect_keys.astype(jnp.float32).reshape(pack_count, blocks, BLOCK, REFL, HEADS, DK))
    key_rows = key_rows.transpose(1, 0, 4, 2, 3, 5).reshape(blocks, pack_count, HEADS, sub_steps, DK)
    value_rows = reflect_values.astype(jnp.float32).reshape(pack_count, blocks, BLOCK, REFL, HEADS, DK)
    value_rows = value_rows.transpose(1, 0, 4, 2, 3, 5).reshape(blocks, pack_count, HEADS, sub_steps, DK)
    beta_rows = reflect_beta.reshape(pack_count, blocks, BLOCK, REFL, HEADS).transpose(1, 0, 4, 2, 3).reshape(blocks, pack_count, HEADS, sub_steps)
    gate_rows = log_decay.reshape(pack_count, blocks, BLOCK, HEADS).transpose(1, 0, 3, 2)
    decay_rows = jnp.concatenate([gate_rows[..., None], jnp.zeros(gate_rows.shape + (REFL - 1,), jnp.float32)], axis=-1).reshape(blocks, pack_count, HEADS, sub_steps)
    seg_rows = jnp.repeat(segment.reshape(pack_count, blocks, BLOCK), REFL, axis=-1).transpose(1, 0, 2).astype(jnp.int32)
    last_row = REFL - 1

    def one_block(carried, inputs):
        state, seg_before = carried
        query_block, key_block, value_block, beta_block, decay_block, seg_block = inputs
        decay_ratio, carry_in, write_vals, write_keys = block_parts(key_block, value_block, beta_block, decay_block, seg_block, seg_before)
        updates = write_vals - jnp.einsum('bhck,bhkv->bhcv', write_keys, state, precision=highest)
        read_weights = decay_ratio[..., last_row::REFL, :] * jnp.einsum('bhik,bhjk->bhij', query_block, key_block, precision=highest)
        carry_read = carry_in[..., last_row::REFL]
        head_out = carry_read[..., None] * jnp.einsum('bhik,bhkv->bhiv', query_block, state, precision=highest) + jnp.einsum('bhij,bhjv->bhiv', read_weights, updates, precision=highest)
        end_keys = decay_ratio[..., -1, :, None] * key_block
        new_state = carry_in[..., -1, None, None] * state + jnp.einsum('bhjk,bhjl->bhkl', end_keys, updates, precision=highest)
        return ((new_state, seg_block[:, -1].astype(jnp.int32)), head_out)
    initial = (jnp.zeros((pack_count, HEADS, DK, DK), jnp.float32), jnp.full((pack_count,), -1, jnp.int32))
    finished, outputs = lax.scan(one_block, initial, (query_rows, key_rows, value_rows, beta_rows, decay_rows, seg_rows))
    outputs = outputs.transpose(1, 0, 3, 2, 4)
    normed = (outputs * lax.rsqrt(lax.optimization_barrier(jnp.mean(outputs * outputs, axis=-1, keepdims=True)) + epsilon) * norm_gain).astype(jnp.bfloat16)
    flat_rows = normed.reshape(pack_count, length, HEADS * DK)
    group_width = HEADS * DK // N_HEAD
    total_sum = jnp.zeros((pack_count, length, out_weight.shape[1]), jnp.float32)
    for group_index in range(N_HEAD):
        lower_col = group_index * group_width
        upper_col = lower_col + group_width
        partial_sum = jnp.dot(flat_rows[..., lower_col:upper_col].astype(jnp.float32), out_weight[lower_col:upper_col].astype(jnp.float32), preferred_element_type=jnp.float32).astype(jnp.bfloat16)
        partial_sum = lax.optimization_barrier(partial_sum)
        total_sum = total_sum + partial_sum.astype(jnp.float32)
    return total_sum.astype(jnp.bfloat16)
```

```python
import functools

import jax
import jax.numpy as jnp
from jax import lax
from jax.experimental import pallas as pl
from jax.experimental.pallas import tpu as pltpu
from jax.sharding import PartitionSpec as P

BLOCK = 64
HEADS_STEP = 2

epsilon = 1e-06
f32 = jnp.float32
bf16 = jnp.bfloat16
highest = lax.Precision.HIGHEST


def mm(a, b):
    return jnp.dot(a, b, preferred_element_type=f32)


def mm_nt(a, b):
    return lax.dot_general(a, b, (((1,), (1,)), ((), ())), preferred_element_type=f32)


def mm_tn(a, b, precision=None):
    return lax.dot_general(
        a, b, (((0,), (0,)), ((), ())), preferred_element_type=f32, precision=precision
    )


def split(x):
    hi = x.astype(bf16)
    return hi, (x - hi.astype(f32)).astype(bf16)


def local_kernel(
    refl, blocks, len_ref, q_ref, k_ref, v_ref, beta_ref, gate_ref,
    oloc_ref, read_ref, add_ref, map_ref, rows_ref,
):
    sub = refl * BLOCK
    width = k_ref.shape[1] // HEADS_STEP
    heads = gate_ref.shape[1]
    tokens = blocks * BLOCK
    step = pl.program_id(0)

    @pl.when(step == 0)
    def _():
        tok = lax.broadcasted_iota(jnp.int32, (tokens, sub), 0)
        lane = lax.broadcasted_iota(jnp.int32, (tokens, sub), 1)
        for b in range(blocks):
            rel = tok - b * BLOCK
            cum = jnp.where((rel >= 0) & (rel <= lane // refl), 1.0, 0.0).astype(f32)
            rows_ref[b, 0] = mm_tn(gate_ref[...], cum, highest)
            total = jnp.zeros((heads, sub), f32)
            for j in range(refl):
                pick = jnp.where(rel * refl + j == lane, 1.0, 0.0).astype(f32)
                pick = jnp.where(rel >= 0, pick, 0.0)
                total += mm_tn(beta_ref[:, j * heads : (j + 1) * heads], pick, highest)
            rows_ref[b, 1] = total

    offset = lax.axis_index("seq") * tokens
    ends = []
    running = 0
    for d in range(len_ref.shape[1]):
        running = running + len_ref[0, d]
        ends.append(running)

    def segment(pos):
        total = jnp.zeros(pos.shape, jnp.int32)
        for end in ends:
            total += jnp.where(pos >= end, 1, 0)
        return total

    row_i = lax.broadcasted_iota(jnp.int32, (sub, sub), 0)
    col_i = lax.broadcasted_iota(jnp.int32, (sub, sub), 1)
    eye = row_i == col_i
    eye_f = jnp.where(eye, 1.0, 0.0).astype(f32)
    tok_i = lax.broadcasted_iota(jnp.int32, (BLOCK, sub), 0)
    tok_j = lax.broadcasted_iota(jnp.int32, (BLOCK, sub), 1)
    pick_tok = tok_j == tok_i * refl + refl - 1
    levels = []
    size = refl
    while size < sub:
        big = min(4 * size, sub)
        levels.append((row_i // big == col_i // big) & (row_i // size > col_i // size))
        size = big

    blocks_geo = []
    for b in range(blocks):
        start = offset + b * BLOCK
        seg_row = segment(start + lax.broadcasted_iota(jnp.int32, (1, sub), 1) // refl)
        seg_col = segment(start + lax.broadcasted_iota(jnp.int32, (sub, 1), 0) // refl)
        seg_tok = segment(start + lax.broadcasted_iota(jnp.int32, (BLOCK, 1), 0))
        before = jnp.where(start == 0, -1, 0)
        last_seg = 0
        for end in ends:
            before += jnp.where(start - 1 >= end, 1, 0)
            last_seg += jnp.where(start + BLOCK - 1 >= end, 1, 0)
        incl = (row_i >= col_i) & (seg_col == seg_row)
        read = (tok_j // refl <= tok_i) & (seg_tok == seg_row)
        blocks_geo.append(
            (incl, read, seg_row == before, seg_tok == before, seg_col == last_seg, last_seg == before)
        )

    for h in range(HEADS_STEP):
        cols = slice(h * width, (h + 1) * width)
        head = step * HEADS_STEP + h
        state = None
        for b in range(blocks):
            incl, read, carry_on, tok_on, end_on, all_on = blocks_geo[b]
            kb = k_ref[b * sub : (b + 1) * sub, cols]
            vb = v_ref[b * sub : (b + 1) * sub, cols]
            qb = q_ref[b * BLOCK : (b + 1) * BLOCK, cols]
            c_row = rows_ref[b, 0, pl.ds(head, 1), :]
            beta_row = rows_ref[b, 1, pl.ds(head, 1), :]
            gram = mm_nt(kb, kb)
            diag = jnp.where(eye, gram, 0.0)
            n_row = lax.rsqrt(jnp.sum(diag, axis=0, keepdims=True) + epsilon)
            n_col = lax.rsqrt(jnp.sum(diag, axis=1, keepdims=True) + epsilon)
            c_col = jnp.sum(jnp.where(eye, c_row, 0.0), axis=1, keepdims=True)
            beta_col = jnp.sum(jnp.where(eye, beta_row, 0.0), axis=1, keepdims=True)
            ratio = jnp.where(incl, jnp.exp(jnp.minimum(c_col - c_row, 0.0)), 0.0)
            low = jnp.where(eye, 0.0, (beta_col * n_col) * ratio * gram * n_row)
            inv = eye_f - jnp.where(row_i // refl == col_i // refl, low, 0.0)
            for mask in levels:
                inv_b = inv.astype(bf16)
                nil = mm(inv_b, jnp.where(mask, low, 0.0).astype(bf16)).astype(bf16)
                both = mm(nil, jnp.concatenate([nil, inv_b], axis=1))
                half = inv - both[:, sub:]
                inv = half + mm(both[:, :sub].astype(bf16), half.astype(bf16))
            inv_b = inv.astype(bf16)
            low_hi, low_lo = split(low)
            resid = eye_f - inv_b.astype(f32) - mm(
                jnp.concatenate([low_hi, low_lo], axis=1), jnp.concatenate([inv_b, inv_b], axis=0)
            )
            inv = inv_b.astype(f32) + mm(inv_b, resid.astype(bf16))
            carry_row = jnp.where(carry_on, jnp.exp(c_row), 0.0)
            tv = jnp.concatenate(split(inv * beta_row), axis=1)
            tk = jnp.concatenate(split(inv * (beta_row * carry_row * n_row)), axis=1)
            kk = jnp.concatenate([kb, kb], axis=0)
            writes = jnp.concatenate([mm(tv, jnp.concatenate([vb, vb], axis=0)), mm(tk, kk)], axis=1)
            c_end = c_row[:, sub - 1 : sub]
            e_col = jnp.where(end_on, jnp.exp(jnp.minimum(c_end - c_col, 0.0)), 0.0) * n_col
            ends_w = jnp.concatenate(split(writes * e_col), axis=0)
            step_w = mm_tn(kk, ends_w)
            carry_end = jnp.where(all_on, jnp.exp(c_end), 0.0)
            block_map = carry_end * eye_f - step_w[:, width:]
            block_add = step_w[:, :width]
            qf = qb.astype(f32)
            nq = lax.rsqrt(jnp.sum(qf * qf, axis=1, keepdims=True) + epsilon) * width ** (-0.5)
            ct = jnp.sum(jnp.where(pick_tok, c_row, 0.0), axis=1, keepdims=True)
            weights = (
                jnp.where(read, jnp.exp(jnp.minimum(ct - c_row, 0.0)), 0.0)
                * mm_nt(qb, kb) * nq * n_row
            )
            reads = mm(weights.astype(bf16), writes.astype(bf16))
            own = reads[:, :width]
            back = (jnp.where(tok_on, jnp.exp(ct), 0.0) * nq) * qf - reads[:, width:]
            if state is None:
                state = jnp.concatenate([block_add, block_map], axis=1)
                out_own, out_back = own, back
            else:
                s_hi, s_lo = split(state)
                m_hi, m_lo = split(block_map)
                moved = mm(back.astype(bf16), s_hi)
                out_own, out_back = own + moved[:, :width], moved[:, width:]
                state = mm(
                    jnp.concatenate([m_hi, m_lo], axis=1), jnp.concatenate([s_hi, s_hi], axis=0)
                ) + mm(m_hi, s_lo)
                state = jnp.concatenate([state[:, :width] + block_add, state[:, width:]], axis=1)
            oloc_ref[b * BLOCK : (b + 1) * BLOCK, cols] = out_own
            read_ref[b * BLOCK : (b + 1) * BLOCK, cols] = out_back.astype(bf16)
        add_ref[h] = state[:, :width]
        map_ref[h] = state[:, width:]


def local_part(lengths, q, k, v, beta, gate):
    tokens, heads = gate.shape
    refl = k.shape[0] // tokens
    width = q.shape[1] // heads
    blocks = tokens // BLOCK
    wide = HEADS_STEP * width
    whole = lambda *shape: pl.BlockSpec(shape, lambda i: (0,) * len(shape))
    column = lambda rows: pl.BlockSpec((rows, wide), lambda i: (0, i))
    square = pl.BlockSpec((HEADS_STEP, width, width), lambda i: (i, 0, 0))
    return pl.pallas_call(
        functools.partial(local_kernel, refl, blocks),
        grid=(heads // HEADS_STEP,),
        in_specs=[
            pl.BlockSpec(memory_space=pltpu.SMEM),
            column(tokens), column(tokens * refl), column(tokens * refl),
            whole(*beta.shape), whole(*gate.shape),
        ],
        out_specs=[column(tokens), column(tokens), square, square],
        out_shape=[
            jax.ShapeDtypeStruct(q.shape, f32),
            jax.ShapeDtypeStruct(q.shape, bf16),
            jax.ShapeDtypeStruct((heads, width, width), f32),
            jax.ShapeDtypeStruct((heads, width, width), f32),
        ],
        scratch_shapes=[pltpu.VMEM((blocks, 2, heads, refl * BLOCK), f32)],
        compiler_params=pltpu.CompilerParams(vmem_limit_bytes=48 * 2**20),
    )(lengths, q, k, v, beta, gate)


def body(queries, reflect_keys, reflect_values, reflect_beta, log_decay, prompt_lengths, norm_gain, out_weight):
    tokens, refl, wide = reflect_keys.shape[1:]
    heads = log_decay.shape[2]
    width = wide // heads
    count = lax.axis_size("seq")
    oloc, read, add, maps = local_part(
        prompt_lengths,
        queries[0],
        reflect_keys[0].reshape(tokens * refl, wide),
        reflect_values[0].reshape(tokens * refl, wide),
        reflect_beta[0].reshape(tokens, refl * heads),
        log_decay[0],
    )
    state = jnp.zeros((heads, width, width), bf16)
    maps_b = maps.astype(bf16)
    for hop in range(count - 1):
        grown = jnp.einsum("hij,hjk->hik", maps_b, state, preferred_element_type=f32) + add
        state = lax.ppermute(grown.astype(bf16), "seq", [(s, s + 1) for s in range(count - 1)])
    out = oloc.reshape(tokens, heads, width) + jnp.einsum(
        "thk,hkv->thv", read.reshape(tokens, heads, width), state, preferred_element_type=f32
    )
    normed = (
        out * lax.rsqrt(jnp.mean(out * out, axis=-1, keepdims=True) + epsilon) * norm_gain
    ).astype(bf16)
    partial = jnp.dot(normed.reshape(tokens, wide), out_weight, preferred_element_type=f32).astype(bf16)
    return lax.psum_scatter(partial, "head", scatter_dimension=0, tiled=True)[None]


def solution(mesh):
    in_specs = (
        P(("parts", "rep"), "seq", "head"),
        P(("parts", "rep"), "seq", None, "head"),
        P(("parts", "rep"), "seq", None, "head"),
        P(("parts", "rep"), "seq", None, "head"),
        P(("parts", "rep"), "seq", "head"),
        P(("parts", "rep"), None),
        P(),
        P("head", None),
    )
    out_specs = P(("parts", "rep"), ("seq", "head"), None)
    return jax.shard_map(body, mesh=mesh, in_specs=in_specs, out_specs=out_specs, check_vma=False)
```

```python
import functools

import jax
import jax.numpy as jnp
from jax import lax
from jax.experimental import pallas as pl
from jax.experimental.pallas import tpu as pltpu
from jax.sharding import PartitionSpec as P

BLOCK = 64
HEADS_STEP = 4
STATE_GROUP = 2
PIECES = 4
MESH = pl.DeviceIdType.MESH

epsilon = 1e-06
f32 = jnp.float32
bf16 = jnp.bfloat16
highest = lax.Precision.HIGHEST


def mm(a, b):
    return jnp.dot(a, b, preferred_element_type=f32)


def mm_nt(a, b):
    return lax.dot_general(a, b, (((1,), (1,)), ((), ())), preferred_element_type=f32)


def mm_tn(a, b, precision=None):
    return lax.dot_general(
        a, b, (((0,), (0,)), ((), ())), preferred_element_type=f32, precision=precision
    )


def split(x):
    hi = x.astype(bf16)
    return hi, (x - hi.astype(f32)).astype(bf16)


def local_kernel(
    refl, blocks, len_ref, q_ref, k_ref, v_ref, beta_ref, gate_ref,
    oloc_ref, read_ref, add_ref, map_ref, rows_ref,
):
    sub = refl * BLOCK
    width = k_ref.shape[1] // HEADS_STEP
    heads = gate_ref.shape[1]
    tokens = blocks * BLOCK
    step = pl.program_id(0)

    @pl.when(step == 0)
    def _():
        tok = lax.broadcasted_iota(jnp.int32, (tokens, sub), 0)
        lane = lax.broadcasted_iota(jnp.int32, (tokens, sub), 1)
        for b in range(blocks):
            rel = tok - b * BLOCK
            cum = jnp.where((rel >= 0) & (rel <= lane // refl), 1.0, 0.0).astype(f32)
            rows_ref[b, 0] = mm_tn(gate_ref[...], cum, highest)
            total = jnp.zeros((heads, sub), f32)
            for j in range(refl):
                pick = jnp.where(rel * refl + j == lane, 1.0, 0.0).astype(f32)
                pick = jnp.where(rel >= 0, pick, 0.0)
                total += mm_tn(beta_ref[:, j * heads : (j + 1) * heads], pick, highest)
            rows_ref[b, 1] = total

    offset = lax.axis_index("seq") * tokens
    ends = []
    running = 0
    for d in range(len_ref.shape[1]):
        running = running + len_ref[0, d]
        ends.append(running)

    def segment(pos):
        total = jnp.zeros(pos.shape, jnp.int32)
        for end in ends:
            total += jnp.where(pos >= end, 1, 0)
        return total

    row_i = lax.broadcasted_iota(jnp.int32, (sub, sub), 0)
    col_i = lax.broadcasted_iota(jnp.int32, (sub, sub), 1)
    eye = row_i == col_i
    eye_f = jnp.where(eye, 1.0, 0.0).astype(f32)
    tok_i = lax.broadcasted_iota(jnp.int32, (BLOCK, sub), 0)
    tok_j = lax.broadcasted_iota(jnp.int32, (BLOCK, sub), 1)
    pick_tok = tok_j == tok_i * refl + refl - 1
    levels = []
    size = refl
    while size < sub:
        big = min(4 * size, sub)
        levels.append((row_i // big == col_i // big) & (row_i // size > col_i // size))
        size = big

    blocks_geo = []
    for b in range(blocks):
        start = offset + b * BLOCK
        seg_row = segment(start + lax.broadcasted_iota(jnp.int32, (1, sub), 1) // refl)
        seg_col = segment(start + lax.broadcasted_iota(jnp.int32, (sub, 1), 0) // refl)
        seg_tok = segment(start + lax.broadcasted_iota(jnp.int32, (BLOCK, 1), 0))
        before = jnp.where(start == 0, -1, 0)
        last_seg = 0
        for end in ends:
            before += jnp.where(start - 1 >= end, 1, 0)
            last_seg += jnp.where(start + BLOCK - 1 >= end, 1, 0)
        incl = (row_i >= col_i) & (seg_col == seg_row)
        read = (tok_j // refl <= tok_i) & (seg_tok == seg_row)
        blocks_geo.append(
            (incl, read, seg_row == before, seg_tok == before, seg_col == last_seg, last_seg == before)
        )

    pairs = [(h, b) for h in range(HEADS_STEP) for b in range(blocks)]

    def over(stage, *lists):
        return [stage(h, b, *args) for (h, b), *args in zip(pairs, *lists)]

    def cols(h):
        return slice(h * width, (h + 1) * width)

    def keys(h, b):
        return k_ref[b * sub : (b + 1) * sub, cols(h)]

    def row(kind, h, b):
        return rows_ref[b, kind, pl.ds(step * HEADS_STEP + h, 1), :]

    def column(values):
        return jnp.sum(jnp.where(eye, values, 0.0), axis=1, keepdims=True)

    def scales(h, b):
        gram = mm_nt(keys(h, b), keys(h, b))
        diag = jnp.where(eye, gram, 0.0)
        n_row = lax.rsqrt(jnp.sum(diag, axis=0, keepdims=True) + epsilon)
        n_col = lax.rsqrt(jnp.sum(diag, axis=1, keepdims=True) + epsilon)
        c_row = row(0, h, b)
        c_col = column(c_row)
        ratio = jnp.where(blocks_geo[b][0], jnp.exp(jnp.minimum(c_col - c_row, 0.0)), 0.0)
        low = jnp.where(eye, 0.0, (column(row(1, h, b)) * n_col) * ratio * gram * n_row)
        return low, n_row, n_col, c_col

    lows, n_rows, n_cols, c_cols = zip(*over(scales))
    invs = [eye_f - jnp.where(row_i // refl == col_i // refl, low, 0.0) for low in lows]
    for mask in levels:
        heads_b = [inv.astype(bf16) for inv in invs]
        nils = [
            mm(inv, jnp.where(mask, low, 0.0).astype(bf16)).astype(bf16)
            for inv, low in zip(heads_b, lows)
        ]
        both = [mm(nil, jnp.concatenate([nil, inv], axis=1)) for nil, inv in zip(nils, heads_b)]
        halves = [inv - pair[:, sub:] for inv, pair in zip(invs, both)]
        invs = [
            half + mm(pair[:, :sub].astype(bf16), half.astype(bf16))
            for half, pair in zip(halves, both)
        ]

    def residual(h, b, inv, low):
        inv_b = inv.astype(bf16)
        low_2 = jnp.concatenate(split(low), axis=1)
        return eye_f - inv_b.astype(f32) - mm(low_2, jnp.concatenate([inv_b, inv_b], axis=0))

    resids = over(residual, invs, lows)

    def refine(h, b, inv, resid):
        inv_b = inv.astype(bf16)
        return inv_b.astype(f32) + mm(inv_b, resid.astype(bf16))

    invs = over(refine, invs, resids)

    def write(h, b, inv, n_row):
        carry_row = jnp.where(blocks_geo[b][2], jnp.exp(row(0, h, b)), 0.0)
        by_beta = inv * row(1, h, b)
        tv = jnp.concatenate(split(by_beta), axis=1)
        tk = jnp.concatenate(split(by_beta * (carry_row * n_row)), axis=1)
        vb, kb = v_ref[b * sub : (b + 1) * sub, cols(h)], keys(h, b)
        return jnp.concatenate(
            [mm(tv, jnp.concatenate([vb, vb], axis=0)), mm(tk, jnp.concatenate([kb, kb], axis=0))],
            axis=1,
        )

    writes = over(write, invs, n_rows)

    def block_step(h, b, wrote, n_col, c_col):
        c_end = row(0, h, b)[:, sub - 1 : sub]
        e_col = jnp.where(blocks_geo[b][4], jnp.exp(jnp.minimum(c_end - c_col, 0.0)), 0.0) * n_col
        kb = keys(h, b)
        moved = mm_tn(
            jnp.concatenate([kb, kb], axis=0), jnp.concatenate(split(wrote * e_col), axis=0)
        )
        carry_end = jnp.where(blocks_geo[b][5], jnp.exp(c_end), 0.0)
        return moved[:, :width], carry_end * eye_f - moved[:, width:]

    steps = over(block_step, writes, n_cols, c_cols)

    def read_weights(h, b, n_row):
        qb, c_row = q_ref[b * BLOCK : (b + 1) * BLOCK, cols(h)], row(0, h, b)
        qf = qb.astype(f32)
        nq = lax.rsqrt(jnp.sum(qf * qf, axis=1, keepdims=True) + epsilon) * width ** (-0.5)
        ct = jnp.sum(jnp.where(pick_tok, c_row, 0.0), axis=1, keepdims=True)
        ratio = jnp.where(blocks_geo[b][1], jnp.exp(jnp.minimum(ct - c_row, 0.0)), 0.0)
        carried = (jnp.where(blocks_geo[b][3], jnp.exp(ct), 0.0) * nq) * qf
        return (ratio * mm_nt(qb, keys(h, b)) * nq * n_row).astype(bf16), carried

    weights = over(read_weights, n_rows)

    def read(h, b, weight, wrote):
        got = mm(weight[0], wrote.astype(bf16))
        return got[:, :width], weight[1] - got[:, width:]

    reads = over(read, weights, writes)

    def emit(h, b, own, back):
        oloc_ref[b * BLOCK : (b + 1) * BLOCK, cols(h)] = own
        read_ref[b * BLOCK : (b + 1) * BLOCK, cols(h)] = back.astype(bf16)

    at = lambda h, b: h * blocks + b
    states = [jnp.concatenate(steps[at(h, 0)], axis=1) for h in range(HEADS_STEP)]
    for h in range(HEADS_STEP):
        emit(h, 0, *reads[at(h, 0)])
    for b in range(1, blocks):
        for h in range(HEADS_STEP):
            block_add, block_map = steps[at(h, b)]
            own, back = reads[at(h, b)]
            s_hi, s_lo = split(states[h])
            m_hi, m_lo = split(block_map)
            moved = mm(back.astype(bf16), s_hi)
            emit(h, b, own + moved[:, :width], moved[:, width:])
            grown = mm(
                jnp.concatenate([m_hi, m_lo], axis=1), jnp.concatenate([s_hi, s_hi], axis=0)
            ) + mm(m_hi, s_lo)
            states[h] = jnp.concatenate([grown[:, :width] + block_add, grown[:, width:]], axis=1)
    for h in range(HEADS_STEP):
        add_ref[h] = states[h][:, :width]
        map_ref[h] = states[h][:, width:]


def local_part(lengths, q, k, v, beta, gate):
    tokens, heads = gate.shape
    refl = k.shape[0] // tokens
    width = q.shape[1] // heads
    blocks = tokens // BLOCK
    wide = HEADS_STEP * width
    whole = lambda *shape: pl.BlockSpec(shape, lambda i: (0,) * len(shape))
    column = lambda rows: pl.BlockSpec((rows, wide), lambda i: (0, i))
    square = pl.BlockSpec((HEADS_STEP, width, width), lambda i: (i, 0, 0))
    return pl.pallas_call(
        functools.partial(local_kernel, refl, blocks),
        grid=(heads // HEADS_STEP,),
        in_specs=[
            pl.BlockSpec(memory_space=pltpu.SMEM),
            column(tokens), column(tokens * refl), column(tokens * refl),
            whole(*beta.shape), whole(*gate.shape),
        ],
        out_specs=[column(tokens), column(tokens), square, square],
        out_shape=[
            jax.ShapeDtypeStruct(q.shape, f32),
            jax.ShapeDtypeStruct(q.shape, bf16),
            jax.ShapeDtypeStruct((heads, width, width), f32),
            jax.ShapeDtypeStruct((heads, width, width), f32),
        ],
        scratch_shapes=[pltpu.VMEM((blocks, 2, heads, refl * BLOCK), f32)],
        compiler_params=pltpu.CompilerParams(vmem_limit_bytes=48 * 2**20),
    )(lengths, q, k, v, beta, gate)


def tail_kernel(
    oloc_ref, read_ref, add_ref, map_ref, gain_ref, weight_hbm, out_ref,
    weight_ref, weight_sem, state_in, state_out, normed_ref, own_ref, part_out, part_in,
    state_send, state_recv, part_send, part_recv,
):
    heads, width = add_ref.shape[:2]
    seq_count, head_count = lax.axis_size("seq"), lax.axis_size("head")
    seq_here, head_here = lax.axis_index("seq"), lax.axis_index("head")
    chunk = out_ref.shape[0]
    first, last = seq_here == 0, seq_here == seq_count - 1
    load = pltpu.make_async_copy(weight_hbm, weight_ref, weight_sem)
    load.start()

    barrier = pltpu.get_barrier_semaphore()

    @pl.when(seq_here > 0)
    def _():
        pl.semaphore_signal(barrier, inc=1, device_id={"seq": seq_here - 1}, device_id_type=MESH)

    @pl.when(seq_here < seq_count - 1)
    def _():
        pl.semaphore_signal(barrier, inc=1, device_id={"seq": seq_here + 1}, device_id_type=MESH)

    others = [lax.rem(head_here + d, head_count) for d in range(1, head_count)]
    for other in others:
        pl.semaphore_signal(barrier, inc=1, device_id={"head": other}, device_id_type=MESH)
    expected = jnp.where(first, 0, 1) + jnp.where(last, 0, 1) + head_count - 1
    pl.semaphore_wait(barrier, expected)

    @pl.when(first)
    def _():
        state_in[...] = jnp.zeros_like(state_in)

    def hop(g):
        part = pl.ds(g * STATE_GROUP, STATE_GROUP)
        return pltpu.make_async_remote_copy(
            src_ref=state_out.at[part],
            dst_ref=state_in.at[part],
            send_sem=state_send.at[g],
            recv_sem=state_recv.at[g],
            device_id={"seq": lax.rem(seq_here + 1, seq_count)},
            device_id_type=MESH,
        )

    for g in range(heads // STATE_GROUP):
        @pl.when(seq_here > 0)
        def _():
            hop(g).wait_recv()

        group = range(g * STATE_GROUP, (g + 1) * STATE_GROUP)

        @pl.when(seq_here < seq_count - 1)
        def _():
            for h in group:
                state = state_in[h]
                both = jnp.concatenate(split(map_ref[h]), axis=1)
                grown = add_ref[h] + mm(both, jnp.concatenate([state, state], axis=0))
                state_out[h] = grown.astype(bf16)
            hop(g).start()

        for h in group:
            cols = slice(h * width, (h + 1) * width)
            out = oloc_ref[:, cols] + mm(read_ref[:, cols], state_in[h])
            scale = lax.rsqrt(jnp.mean(out * out, axis=-1, keepdims=True) + epsilon)
            normed_ref[:, cols] = (out * scale * gain_ref[...]).astype(bf16)

    load.wait()
    piece = weight_ref.shape[1] // PIECES
    copies = []
    for slot, other in enumerate(others):
        rows = normed_ref[pl.ds(pl.multiple_of(other * chunk, chunk), chunk), :]
        for p in range(PIECES):
            cols = pl.ds(p * piece, piece)
            part_out[slot, :, cols] = mm(rows, weight_ref[:, cols]).astype(bf16)
            copies.append(
                pltpu.make_async_remote_copy(
                    src_ref=part_out.at[slot, :, cols],
                    dst_ref=part_in.at[slot, :, cols],
                    send_sem=part_send.at[slot, p],
                    recv_sem=part_recv.at[slot, p],
                    device_id={"head": other},
                    device_id_type=MESH,
                )
            )
            copies[-1].start()
    rows = normed_ref[pl.ds(pl.multiple_of(head_here * chunk, chunk), chunk), :]
    for p in range(PIECES):
        cols = pl.ds(p * piece, piece)
        own_ref[:, cols] = mm(rows, weight_ref[:, cols])
    for p in range(PIECES):
        cols = pl.ds(p * piece, piece)
        total = own_ref[:, cols].astype(bf16).astype(f32)
        for slot in range(len(others)):
            copies[slot * PIECES + p].wait_recv()
            total += part_in[slot, :, cols].astype(f32)
        out_ref[:, cols] = total.astype(bf16)
    for copy in copies:
        copy.wait_send()

    @pl.when(seq_here < seq_count - 1)
    def _():
        for g in range(heads // STATE_GROUP):
            hop(g).wait_send()


def tail_part(oloc, read, add, maps, gain, weight):
    tokens, wide = oloc.shape
    heads, width = add.shape[:2]
    head_count = lax.axis_size("head")
    chunk, model = tokens // head_count, weight.shape[1]
    groups = heads // STATE_GROUP
    slots = max(head_count - 1, 1)
    vmem = pl.BlockSpec(memory_space=pltpu.VMEM)
    return pl.pallas_call(
        tail_kernel,
        in_specs=[vmem] * 5 + [pl.BlockSpec(memory_space=pl.ANY)],
        out_specs=vmem,
        out_shape=jax.ShapeDtypeStruct((chunk, model), bf16),
        scratch_shapes=[
            pltpu.VMEM(weight.shape, bf16),
            pltpu.SemaphoreType.DMA,
            pltpu.VMEM((heads, width, width), bf16),
            pltpu.VMEM((heads, width, width), bf16),
            pltpu.VMEM((tokens, wide), bf16),
            pltpu.VMEM((chunk, model), f32),
            pltpu.VMEM((slots, chunk, model), bf16),
            pltpu.VMEM((slots, chunk, model), bf16),
            pltpu.SemaphoreType.DMA((groups,)),
            pltpu.SemaphoreType.DMA((groups,)),
            pltpu.SemaphoreType.DMA((slots, PIECES)),
            pltpu.SemaphoreType.DMA((slots, PIECES)),
        ],
        compiler_params=pltpu.CompilerParams(
            collective_id=0, has_side_effects=True, vmem_limit_bytes=32 * 2**20
        ),
    )(oloc, read, add, maps, gain, weight)


def body(queries, reflect_keys, reflect_values, reflect_beta, log_decay, prompt_lengths, norm_gain, out_weight):
    tokens, refl, wide = reflect_keys.shape[1:]
    heads = log_decay.shape[2]
    oloc, read, add, maps = local_part(
        prompt_lengths,
        queries[0],
        reflect_keys[0].reshape(tokens * refl, wide),
        reflect_values[0].reshape(tokens * refl, wide),
        reflect_beta[0].reshape(tokens, refl * heads),
        log_decay[0],
    )
    return tail_part(oloc, read, add, maps, norm_gain[None], out_weight)[None]


def solution(mesh):
    in_specs = (
        P(("parts", "rep"), "seq", "head"),
        P(("parts", "rep"), "seq", None, "head"),
        P(("parts", "rep"), "seq", None, "head"),
        P(("parts", "rep"), "seq", None, "head"),
        P(("parts", "rep"), "seq", "head"),
        P(("parts", "rep"), None),
        P(),
        P("head", None),
    )
    out_specs = P(("parts", "rep"), ("seq", "head"), None)
    return jax.shard_map(body, mesh=mesh, in_specs=in_specs, out_specs=out_specs, check_vma=False)
```

```python
import functools

import jax
import jax.numpy as jnp
from jax import lax
from jax.experimental import pallas as pl
from jax.experimental.pallas import tpu as pltpu
from jax.sharding import PartitionSpec as P

BLOCK = 64
HEADS_STEP = 4
STATE_GROUP = 2
PIECES = 4
MESH = pl.DeviceIdType.MESH

epsilon = 1e-06
f32 = jnp.float32
bf16 = jnp.bfloat16
highest = lax.Precision.HIGHEST


def mm(a, b, precision=None):
    return jnp.dot(a, b, preferred_element_type=f32, precision=precision)


def mm_nt(a, b):
    return lax.dot_general(a, b, (((1,), (1,)), ((), ())), preferred_element_type=f32)


def mm_tn(a, b):
    return lax.dot_general(a, b, (((0,), (0,)), ((), ())), preferred_element_type=f32)


def split(x):
    hi = x.astype(bf16)
    return hi, (x - hi.astype(f32)).astype(bf16)


def local_kernel(
    refl, blocks, len_ref, q_ref, k_ref, v_ref, beta_ref, gate_ref,
    oloc_ref, read_ref, add_ref, map_ref, rows_ref,
):
    sub = refl * BLOCK
    width = k_ref.shape[1] // HEADS_STEP
    heads = gate_ref.shape[0]
    tokens = blocks * BLOCK
    step = pl.program_id(0)

    @pl.when(step == 0)
    def _():
        tok = lax.broadcasted_iota(jnp.int32, (tokens, sub), 0)
        lane = lax.broadcasted_iota(jnp.int32, (tokens, sub), 1)
        for b in range(blocks):
            rel = tok - b * BLOCK
            cum = jnp.where((rel >= 0) & (rel <= lane // refl), 1.0, 0.0).astype(f32)
            rows_ref[b, 0] = mm(gate_ref[...], cum, highest)
            total = jnp.zeros((heads, sub), f32)
            for j in range(refl):
                pick = jnp.where(rel * refl + j == lane, 1.0, 0.0).astype(f32)
                pick = jnp.where(rel >= 0, pick, 0.0)
                total += mm(beta_ref[j], pick, highest)
            rows_ref[b, 1] = total

    offset = lax.axis_index("seq") * tokens
    ends = []
    running = 0
    for d in range(len_ref.shape[1]):
        running = running + len_ref[0, d]
        ends.append(running)

    def segment(pos):
        total = jnp.zeros(pos.shape, jnp.int32)
        for end in ends:
            total += jnp.where(pos >= end, 1, 0)
        return total

    row_i = lax.broadcasted_iota(jnp.int32, (sub, sub), 0)
    col_i = lax.broadcasted_iota(jnp.int32, (sub, sub), 1)
    eye = row_i == col_i
    eye_f = jnp.where(eye, 1.0, 0.0).astype(f32)
    tok_i = lax.broadcasted_iota(jnp.int32, (BLOCK, sub), 0)
    tok_j = lax.broadcasted_iota(jnp.int32, (BLOCK, sub), 1)
    pick_tok = tok_j == tok_i * refl + refl - 1
    levels = []
    size = refl
    while size < sub:
        big = min(4 * size, sub)
        levels.append((row_i // big == col_i // big) & (row_i // size > col_i // size))
        size = big

    blocks_geo = []
    for b in range(blocks):
        start = offset + b * BLOCK
        seg_row = segment(start + lax.broadcasted_iota(jnp.int32, (1, sub), 1) // refl)
        seg_col = segment(start + lax.broadcasted_iota(jnp.int32, (sub, 1), 0) // refl)
        seg_tok = segment(start + lax.broadcasted_iota(jnp.int32, (BLOCK, 1), 0))
        before = jnp.where(start == 0, -1, 0)
        last_seg = 0
        for end in ends:
            before += jnp.where(start - 1 >= end, 1, 0)
            last_seg += jnp.where(start + BLOCK - 1 >= end, 1, 0)
        incl = (row_i >= col_i) & (seg_col == seg_row)
        read = (tok_j // refl <= tok_i) & (seg_tok == seg_row)
        blocks_geo.append(
            (incl, read, seg_row == before, seg_tok == before, seg_col == last_seg, last_seg == before)
        )

    pairs = [(h, b) for h in range(HEADS_STEP) for b in range(blocks)]

    def over(stage, *lists):
        return [stage(h, b, *args) for (h, b), *args in zip(pairs, *lists)]

    def cols(h):
        return slice(h * width, (h + 1) * width)

    def keys(h, b):
        return k_ref[b * sub : (b + 1) * sub, cols(h)]

    def row(kind, h, b):
        return rows_ref[b, kind, pl.ds(step * HEADS_STEP + h, 1), :]

    def column(values):
        return jnp.sum(jnp.where(eye, values, 0.0), axis=1, keepdims=True)

    def scales(h, b):
        gram = mm_nt(keys(h, b), keys(h, b))
        diag = jnp.where(eye, gram, 0.0)
        n_row = lax.rsqrt(jnp.sum(diag, axis=0, keepdims=True) + epsilon)
        n_col = lax.rsqrt(jnp.sum(diag, axis=1, keepdims=True) + epsilon)
        c_row = row(0, h, b)
        c_col = column(c_row)
        ratio = jnp.where(blocks_geo[b][0], jnp.exp(jnp.minimum(c_col - c_row, 0.0)), 0.0)
        low = jnp.where(eye, 0.0, (column(row(1, h, b)) * n_col) * ratio * gram * n_row)
        return low, n_row, n_col, c_col

    lows, n_rows, n_cols, c_cols = zip(*over(scales))
    invs = [eye_f - jnp.where(row_i // refl == col_i // refl, low, 0.0) for low in lows]
    for mask in levels:
        heads_b = [inv.astype(bf16) for inv in invs]
        nils = [
            mm(inv, jnp.where(mask, low, 0.0).astype(bf16)).astype(bf16)
            for inv, low in zip(heads_b, lows)
        ]
        both = [mm(nil, jnp.concatenate([nil, inv], axis=1)) for nil, inv in zip(nils, heads_b)]
        halves = [inv - pair[:, sub:] for inv, pair in zip(invs, both)]
        invs = [
            half + mm(pair[:, :sub].astype(bf16), half.astype(bf16))
            for half, pair in zip(halves, both)
        ]

    def residual(h, b, inv, low):
        inv_b = inv.astype(bf16)
        low_2 = jnp.concatenate(split(low), axis=1)
        return eye_f - inv_b.astype(f32) - mm(low_2, jnp.concatenate([inv_b, inv_b], axis=0))

    resids = over(residual, invs, lows)

    def refine(h, b, inv, resid):
        inv_b = inv.astype(bf16)
        return inv_b.astype(f32) + mm(inv_b, resid.astype(bf16))

    invs = over(refine, invs, resids)

    def write(h, b, inv, n_row):
        carry_row = jnp.where(blocks_geo[b][2], jnp.exp(row(0, h, b)), 0.0)
        by_beta = inv * row(1, h, b)
        tv = jnp.concatenate(split(by_beta), axis=1)
        tk = jnp.concatenate(split(by_beta * (carry_row * n_row)), axis=1)
        vb, kb = v_ref[b * sub : (b + 1) * sub, cols(h)], keys(h, b)
        return jnp.concatenate(
            [mm(tv, jnp.concatenate([vb, vb], axis=0)), mm(tk, jnp.concatenate([kb, kb], axis=0))],
            axis=1,
        )

    writes = over(write, invs, n_rows)

    def block_step(h, b, wrote, n_col, c_col):
        c_end = row(0, h, b)[:, sub - 1 : sub]
        e_col = jnp.where(blocks_geo[b][4], jnp.exp(jnp.minimum(c_end - c_col, 0.0)), 0.0) * n_col
        kb = keys(h, b)
        moved = mm_tn(
            jnp.concatenate([kb, kb], axis=0), jnp.concatenate(split(wrote * e_col), axis=0)
        )
        carry_end = jnp.where(blocks_geo[b][5], jnp.exp(c_end), 0.0)
        return moved[:, :width], carry_end * eye_f - moved[:, width:]

    steps = over(block_step, writes, n_cols, c_cols)

    def read_weights(h, b, n_row):
        qb, c_row = q_ref[b * BLOCK : (b + 1) * BLOCK, cols(h)], row(0, h, b)
        qf = qb.astype(f32)
        nq = lax.rsqrt(jnp.sum(qf * qf, axis=1, keepdims=True) + epsilon) * width ** (-0.5)
        ct = jnp.sum(jnp.where(pick_tok, c_row, 0.0), axis=1, keepdims=True)
        ratio = jnp.where(blocks_geo[b][1], jnp.exp(jnp.minimum(ct - c_row, 0.0)), 0.0)
        carried = (jnp.where(blocks_geo[b][3], jnp.exp(ct), 0.0) * nq) * qf
        return (ratio * mm_nt(qb, keys(h, b)) * nq * n_row).astype(bf16), carried

    weights = over(read_weights, n_rows)

    def read(h, b, weight, wrote):
        got = mm(weight[0], wrote.astype(bf16))
        return got[:, :width], weight[1] - got[:, width:]

    reads = over(read, weights, writes)

    def emit(h, b, own, back):
        oloc_ref[step, b * BLOCK : (b + 1) * BLOCK, cols(h)] = own
        read_ref[step, b * BLOCK : (b + 1) * BLOCK, cols(h)] = back.astype(bf16)

    at = lambda h, b: h * blocks + b
    states = [jnp.concatenate(steps[at(h, 0)], axis=1) for h in range(HEADS_STEP)]
    for h in range(HEADS_STEP):
        emit(h, 0, *reads[at(h, 0)])
    for b in range(1, blocks):
        for h in range(HEADS_STEP):
            block_add, block_map = steps[at(h, b)]
            own, back = reads[at(h, b)]
            s_hi, s_lo = split(states[h])
            m_hi, m_lo = split(block_map)
            moved = mm(back.astype(bf16), s_hi)
            emit(h, b, own + moved[:, :width], moved[:, width:])
            grown = mm(
                jnp.concatenate([m_hi, m_lo], axis=1), jnp.concatenate([s_hi, s_hi], axis=0)
            ) + mm(m_hi, s_lo)
            states[h] = jnp.concatenate([grown[:, :width] + block_add, grown[:, width:]], axis=1)
    for h in range(HEADS_STEP):
        add_ref[step * HEADS_STEP + h] = states[h][:, :width]
        map_ref[step * HEADS_STEP + h] = states[h][:, width:]


def mixer_kernel(
    refl, blocks, len_ref, q_ref, k_ref, v_ref, beta_ref, gate_ref, gain_ref, weight_hbm, out_ref,
    rows_ref, oloc_ref, read_ref, add_ref, map_ref,
    weight_ref, weight_sem, state_in, state_out, normed_ref, own_ref, part_out, part_in,
    state_send, state_recv, part_send, part_recv,
):
    heads, width = add_ref.shape[:2]
    step, steps = pl.program_id(0), heads // HEADS_STEP
    groups = heads // STATE_GROUP
    seq_count, head_count = lax.axis_size("seq"), lax.axis_size("head")
    seq_here, head_here = lax.axis_index("seq"), lax.axis_index("head")
    chunk = out_ref.shape[0]
    first, last = seq_here == 0, seq_here == seq_count - 1
    others = [lax.rem(head_here + d, head_count) for d in range(1, head_count)]
    load = pltpu.make_async_copy(weight_hbm, weight_ref, weight_sem)

    @pl.when(step == 0)
    def _():
        load.start()
        barrier = pltpu.get_barrier_semaphore()

        @pl.when(seq_here > 0)
        def _():
            pl.semaphore_signal(barrier, inc=1, device_id={"seq": seq_here - 1}, device_id_type=MESH)

        @pl.when(seq_here < seq_count - 1)
        def _():
            pl.semaphore_signal(barrier, inc=1, device_id={"seq": seq_here + 1}, device_id_type=MESH)

        for other in others:
            pl.semaphore_signal(barrier, inc=1, device_id={"head": other}, device_id_type=MESH)

    local_kernel(
        refl, blocks, len_ref, q_ref, k_ref, v_ref, beta_ref, gate_ref,
        oloc_ref, read_ref, add_ref, map_ref, rows_ref,
    )

    @pl.when(step == 0)
    def _():
        expected = jnp.where(first, 0, 1) + jnp.where(last, 0, 1) + head_count - 1
        pl.semaphore_wait(pltpu.get_barrier_semaphore(), expected)

        @pl.when(first)
        def _():
            state_in[...] = jnp.zeros_like(state_in)

    def hop(g):
        part = pl.ds(g * STATE_GROUP, STATE_GROUP)
        return pltpu.make_async_remote_copy(
            src_ref=state_out.at[part],
            dst_ref=state_in.at[part],
            send_sem=state_send.at[g],
            recv_sem=state_recv.at[g],
            device_id={"seq": lax.rem(seq_here + 1, seq_count)},
            device_id_type=MESH,
        )

    @pl.when((seq_here == 0) & (seq_here < seq_count - 1))
    def _():
        for g in range(HEADS_STEP // STATE_GROUP):
            here = step * (HEADS_STEP // STATE_GROUP) + g
            for h in range(STATE_GROUP):
                state_out[here * STATE_GROUP + h] = add_ref[here * STATE_GROUP + h].astype(bf16)
            hop(here).start()

    @pl.when(step == steps - 1)
    def _():
        for g in range(groups):
            group = range(g * STATE_GROUP, (g + 1) * STATE_GROUP)

            @pl.when(seq_here > 0)
            def _():
                hop(g).wait_recv()

            @pl.when((seq_here > 0) & (seq_here < seq_count - 1))
            def _():
                for h in group:
                    state = state_in[h]
                    both = jnp.concatenate(split(map_ref[h]), axis=1)
                    grown = add_ref[h] + mm(both, jnp.concatenate([state, state], axis=0))
                    state_out[h] = grown.astype(bf16)
                hop(g).start()

            for h in group:
                cols = slice(h * width, (h + 1) * width)
                at, local = h // HEADS_STEP, slice(h % HEADS_STEP * width, (h % HEADS_STEP + 1) * width)
                out = oloc_ref[at, :, local] + mm(read_ref[at, :, local], state_in[h])
                scale = lax.rsqrt(jnp.mean(out * out, axis=-1, keepdims=True) + epsilon)
                normed_ref[:, cols] = (out * scale * gain_ref[...]).astype(bf16)

        load.wait()
        piece = weight_ref.shape[1] // PIECES
        copies = []
        for slot, other in enumerate(others):
            rows = normed_ref[pl.ds(pl.multiple_of(other * chunk, chunk), chunk), :]
            for p in range(PIECES):
                cols = pl.ds(p * piece, piece)
                part_out[slot, :, cols] = mm(rows, weight_ref[:, cols]).astype(bf16)
                copies.append(
                    pltpu.make_async_remote_copy(
                        src_ref=part_out.at[slot, :, cols],
                        dst_ref=part_in.at[slot, :, cols],
                        send_sem=part_send.at[slot, p],
                        recv_sem=part_recv.at[slot, p],
                        device_id={"head": other},
                        device_id_type=MESH,
                    )
                )
                copies[-1].start()
        rows = normed_ref[pl.ds(pl.multiple_of(head_here * chunk, chunk), chunk), :]
        for p in range(PIECES):
            cols = pl.ds(p * piece, piece)
            own_ref[:, cols] = mm(rows, weight_ref[:, cols])
        for p in range(PIECES):
            cols = pl.ds(p * piece, piece)
            total = own_ref[:, cols].astype(bf16).astype(f32)
            for slot in range(len(others)):
                copies[slot * PIECES + p].wait_recv()
                total += part_in[slot, :, cols].astype(f32)
            out_ref[:, cols] = total.astype(bf16)
        for copy in copies:
            copy.wait_send()

        @pl.when(seq_here < seq_count - 1)
        def _():
            for g in range(groups):
                hop(g).wait_send()


def body(queries, reflect_keys, reflect_values, reflect_beta, log_decay, prompt_lengths, norm_gain, out_weight):
    tokens, refl, wide = reflect_keys.shape[1:]
    heads = log_decay.shape[2]
    width = wide // heads
    blocks = tokens // BLOCK
    head_count = lax.axis_size("head")
    chunk, model = tokens // head_count, out_weight.shape[1]
    groups, steps, slots = heads // STATE_GROUP, heads // HEADS_STEP, max(head_count - 1, 1)
    wide_step = HEADS_STEP * width
    beta, gate = reflect_beta[0].transpose(1, 2, 0), log_decay[0].T
    whole = lambda shape: pl.BlockSpec(shape, lambda i: (0,) * len(shape))
    column = lambda rows: pl.BlockSpec((rows, wide_step), lambda i: (0, i))
    dma = pltpu.SemaphoreType.DMA
    out = pl.pallas_call(
        functools.partial(mixer_kernel, refl, blocks),
        grid=(steps,),
        in_specs=[
            pl.BlockSpec(memory_space=pltpu.SMEM),
            column(tokens), column(tokens * refl), column(tokens * refl),
            whole(beta.shape), whole(gate.shape), whole((1, width)),
            pl.BlockSpec(memory_space=pl.ANY),
        ],
        out_specs=whole((chunk, model)),
        out_shape=jax.ShapeDtypeStruct((chunk, model), bf16),
        scratch_shapes=[
            pltpu.VMEM((blocks, 2, heads, refl * BLOCK), f32),
            pltpu.VMEM((steps, tokens, wide_step), f32),
            pltpu.VMEM((steps, tokens, wide_step), bf16),
            pltpu.VMEM((heads, width, width), f32),
            pltpu.VMEM((heads, width, width), f32),
            pltpu.VMEM(out_weight.shape, bf16),
            dma,
            pltpu.VMEM((heads, width, width), bf16),
            pltpu.VMEM((heads, width, width), bf16),
            pltpu.VMEM((tokens, wide), bf16),
            pltpu.VMEM((chunk, model), f32),
            pltpu.VMEM((slots, chunk, model), bf16),
            pltpu.VMEM((slots, chunk, model), bf16),
            dma((groups,)), dma((groups,)), dma((slots, PIECES)), dma((slots, PIECES)),
        ],
        compiler_params=pltpu.CompilerParams(
            collective_id=0, has_side_effects=True, vmem_limit_bytes=56 * 2**20
        ),
    )(
        prompt_lengths,
        queries[0],
        reflect_keys[0].reshape(tokens * refl, wide),
        reflect_values[0].reshape(tokens * refl, wide),
        beta,
        gate,
        norm_gain[None],
        out_weight,
    )
    return out[None]


def solution(mesh):
    in_specs = (
        P(("parts", "rep"), "seq", "head"),
        P(("parts", "rep"), "seq", None, "head"),
        P(("parts", "rep"), "seq", None, "head"),
        P(("parts", "rep"), "seq", None, "head"),
        P(("parts", "rep"), "seq", "head"),
        P(("parts", "rep"), None),
        P(),
        P("head", None),
    )
    out_specs = P(("parts", "rep"), ("seq", "head"), None)
    return jax.shard_map(body, mesh=mesh, in_specs=in_specs, out_specs=out_specs, check_vma=False)
```
